256 devices in a mesh: blk: 64 (over y, x_hi, z), grp: 4 (over x_lo, core).
Axes of the slice: x: 4 (x_hi: 2, x_lo: 2; x = x_hi * 2 + x_lo), y: 4, z: 8, core: 2. Of those that a mesh axis runs over, the one named last changes fastest.
Arguments:
- hidden: bfloat16 [524288, 384], P(('blk', 'grp')), may hold values from -6 to 6
- cotangent: bfloat16 [524288, 384], P(('blk', 'grp')), may hold values from -6 to 6
- token_ids: int32 [524288], P(('blk', 'grp')), may hold values from 0 to 32127, as said below
- w_in: bfloat16 [64, 4, 384, 1536], P('blk', 'grp'), may hold values from -6 to 6
- w_out: bfloat16 [1536, 384], replicated, may hold values from -0.15625 to 0.15625
- tracker: bfloat16 [64, 4, 384, 1536], P('blk', 'grp'), may hold values from -6 to 6
- grad_old: bfloat16 [64, 4, 384, 1536], P('blk', 'grp'), may hold values from -6 to 6
- cheb_num: int32 [4], replicated, may hold values from 10 to 16
- cheb_den: int32 [4], replicated, may hold values from 9 to 11
Outputs:
- new_params: bfloat16 [64, 4, 384, 1536], P('blk', 'grp')
- new_tracker: bfloat16 [64, 4, 384, 1536], P('blk', 'grp')
The draws below stay inside these ranges and needn't reach their ends.
Inputs may be any that keep to these rules, and one draw needn't show every extreme that they name: `token_ids`: each aligned run of 512 rows is one sequence: ids from 1 to 32127 up to its length, 0 after it; every length is 128 or more.
All inputs are finite; a program needn't handle non-finite values.
Results may differ from the reference program's by a relative error of at most 0.013.
Values may be sent and summed in bfloat16 or wider, within the bound.
No kernel may reach another device: no remote copies, remote signals or barrier semaphores. Data moves between devices by JAX's collectives and lax.ppermute only.
A program may use at most 128 MiB of HBM per device.

```python
import math
import jax
import jax.numpy as jnp
from jax import lax

D = 384
FF = 1536
VOCAB = 32128
SEQ_LEN = 512
ROUNDS = 4
TOK_DEV = 2048
TOKENS = 524288
N_BLK = 64
N_GRP = 4


def draw_token_ids(key, part):
    base_key = jax.random.fold_in(key, 7)
    length_key, value_key = jax.random.split(base_key)
    count = TOKENS // SEQ_LEN
    lengths = jax.random.randint(length_key, (count, 1), SEQ_LEN // 4, SEQ_LEN + 1)
    values = jax.random.randint(value_key, (count, SEQ_LEN), 1, VOCAB)
    position = jnp.arange(SEQ_LEN, dtype=jnp.int32)[None, :]
    return jnp.where(position < lengths, values, 0).astype(jnp.int32).reshape(TOKENS)


def with_ends(entries, stream_key, low, largest):
    place = [jax.random.randint(jax.random.fold_in(stream_key, axis), (), 0, length) for axis, length in enumerate(entries.shape)]
    widest = entries.shape.index(max(entries.shape))
    next_to = place[:widest] + [(place[widest] + 1) % entries.shape[widest]] + place[widest + 1:]
    return entries.at[tuple(place)].set(low).at[tuple(next_to)].set(largest)


def levels(rng, shape, cuts, least, largest):
    def one(dim, blocks):
        heights = jax.random.uniform(jax.random.fold_in(jax.random.fold_in(rng, 6), dim), (blocks,), jnp.float32, least / len(cuts), largest / len(cuts))
        return jnp.repeat(jnp.exp(heights), shape[dim] // blocks).reshape((-1,) + (1,) * (len(shape) - dim - 1))

    factor_of = one(*cuts[0])
    for cut in cuts[1:]:
        factor_of = factor_of * one(*cut)
    return factor_of


def normal_values(key, extent, deviation, bound, cuts=(), held_as=jnp.bfloat16):
    values = jax.random.normal(key, extent, jnp.float32) * deviation
    if len(cuts) > 0:
        values = levels(key, extent, cuts, -0.22, 0.18) * values
    return jnp.clip(values, min=-bound, max=bound).astype(held_as)


def setup_inputs(seed: int = 0) -> dict:
    arg_keys = jax.random.split(jax.random.key(seed), 10)
    return {
        "hidden": normal_values(arg_keys[0], (TOKENS, D), 1.0, 6.0, ((0, 256),)),
        "cotangent": normal_values(arg_keys[1], (TOKENS, D), 1.0, 6.0, ((0, 256),)),
        "token_ids": draw_token_ids(jax.random.fold_in(arg_keys[9], 71), 0),
        "w_in": normal_values(arg_keys[3], (N_BLK, N_GRP, D, FF), 1.0, 6.0, ((0, 64), (1, 4))),
        "w_out": normal_values(arg_keys[4], (FF, D), FF ** -0.5, 0.15625),
        "tracker": normal_values(arg_keys[5], (N_BLK, N_GRP, D, FF), 0.5, 6.0, ((0, 64), (1, 4))),
        "grad_old": normal_values(arg_keys[6], (N_BLK, N_GRP, D, FF), 0.5, 6.0, ((0, 64), (1, 4))),
        "cheb_num": with_ends(jax.random.randint(arg_keys[7], (ROUNDS,), 10, 17), jax.random.fold_in(arg_keys[7], 1), 10, 16).astype(jnp.int32),
        "cheb_den": with_ends(jax.random.randint(arg_keys[8], (ROUNDS,), 9, 12), jax.random.fold_in(arg_keys[8], 1), 9, 11).astype(jnp.int32),
    }


epsilon = 1e-06
step_size = 0.25
tanh_scale = math.sqrt(2.0 / math.pi)

def gelu_slope(values):
    cubic = values * values * values
    bent_tanh = jnp.tanh(tanh_scale * (values + 0.044715 * cubic))
    return 0.5 * (1.0 + bent_tanh) + 0.5 * values * (1.0 - bent_tanh * bent_tanh) * tanh_scale * (1.0 + 3.0 * 0.044715 * values * values)

def cycle(field):
    return (jnp.roll(field, 1, 0) + field + jnp.roll(field, -1, 0)) / 3.0

def local_grad(packed, w_out):
    rows, grads_in, ids_rows, params = packed
    widened = rows.astype(jnp.float32)
    mean_square = lax.optimization_barrier(jnp.mean(widened * widened, axis=-1, keepdims=True))
    normed = (widened * lax.rsqrt(mean_square + epsilon)).astype(jnp.bfloat16)
    inv_root = params.shape[0] ** (-0.5)
    pre_act = jnp.dot(normed, params, preferred_element_type=jnp.float32) * inv_root
    masked = jnp.where((ids_rows != 0)[:, None], grads_in, jnp.zeros_like(grads_in))
    back_flow = lax.dot_general(masked, w_out, (((1,), (1,)), ((), ())), preferred_element_type=jnp.float32)
    slope_bf = (back_flow * gelu_slope(pre_act)).astype(jnp.bfloat16)
    return lax.dot_general(normed, slope_bf, (((0,), (0,)), ((), ())), preferred_element_type=jnp.float32) * inv_root

def reference(hidden, cotangent, token_ids, w_in, w_out, tracker, grad_old, cheb_num, cheb_den):
    cycle_mixed = cycle(w_in.astype(jnp.float32))
    mixed_params = lax.optimization_barrier(jnp.sum(cycle_mixed, axis=1, keepdims=True)) / N_GRP
    new_params = (mixed_params - step_size * tracker.astype(jnp.float32)).astype(jnp.bfloat16)
    weights = cheb_num.astype(jnp.float32) / cheb_den.astype(jnp.float32)
    older_iter = tracker.astype(jnp.float32)
    current = older_iter
    for turn_idx in range(ROUNDS):
        next_iter = weights[turn_idx] * cycle(current) + (1.0 - weights[turn_idx]) * older_iter
        older_iter, current = (current, next_iter)
    workers = N_BLK * N_GRP
    packed = (hidden.reshape(workers, TOK_DEV, D), cotangent.reshape(workers, TOK_DEV, D), token_ids.reshape(workers, TOK_DEV), new_params.reshape(workers, D, FF))
    grad_new = lax.map(lambda item: local_grad(item, w_out), packed).reshape(N_BLK, N_GRP, D, FF)
    new_tracker = (current + grad_new - grad_old.astype(jnp.float32)).astype(jnp.bfloat16)
    return (new_params, new_tracker)
```

```python
import math

import jax
import jax.numpy as jnp
from jax import lax
from jax.experimental import pallas as pl
from jax.experimental.pallas import tpu as pltpu
from jax.sharding import PartitionSpec as P


ROUNDS = 4

epsilon = 1e-06
step_size = 0.25
tanh_scale = math.sqrt(2.0 / math.pi)

f32 = jnp.float32
bf16 = jnp.bfloat16


def slope_of(scaled, back_flow, inv_root):
    lead, bend = tanh_scale * inv_root, tanh_scale * 0.044715 * inv_root**3
    square = scaled * scaled
    half = 0.5 * jnp.tanh(scaled * (lead + bend * square)) + 0.5
    inner = scaled * (2.0 * lead + 6.0 * bend * square)
    return back_flow * (half + half * (1.0 - half) * inner)


def grad_body(
    place_ref,
    normed_ref,
    turned_ref,
    masked_ref,
    first_ref,
    second_ref,
    third_ref,
    fourth_ref,
    tracker_ref,
    w_out_ref,
    old_ref,
    params_ref,
    out_ref,
    mixed_ref,
    slope_ref,
):
    tokens, width = normed_ref.shape
    inv_root = width ** (-0.5)
    quarter = width // 4
    for k, part_ref in enumerate((first_ref, second_ref, third_ref, fourth_ref)):
        at = pl.multiple_of(place_ref[k] * quarter, quarter)
        mixed_ref[pl.ds(at, quarter)] = part_ref[...]
    params_ref[...] = (
        mixed_ref[...].astype(f32) - step_size * tracker_ref[...].astype(f32)
    ).astype(bf16)
    step = 256
    held = None
    for at in range(0, tokens + step, step):
        ready = held
        if at < tokens:
            rows = pl.ds(at, step)
            scaled = jnp.dot(normed_ref[rows], params_ref[...], preferred_element_type=f32)
            back_flow = lax.dot_general(
                masked_ref[rows],
                w_out_ref[...],
                (((1,), (1,)), ((), ())),
                preferred_element_type=f32,
            )
            held = (rows, scaled, back_flow)
        if ready is not None:
            rows, scaled, back_flow = ready
            slope_ref[rows] = slope_of(scaled, back_flow, inv_root).astype(bf16)
    grad = jnp.dot(turned_ref[...], slope_ref[...], preferred_element_type=f32)
    out_ref[...] = grad * inv_root - old_ref[...].astype(f32)


def grad_change(place, normed, turned, masked, parts, tracker, w_out, grad_old):
    tokens, width = normed.shape
    hidden = tracker.shape[1]
    block = 256
    whole = pl.BlockSpec(memory_space=pltpu.VMEM)
    column = pl.BlockSpec((width, block), lambda j: (0, j))
    piece = pl.BlockSpec((width // 4, block), lambda j: (0, j))
    return pl.pallas_call(
        grad_body,
        grid=(hidden // block,),
        out_shape=(
            jax.ShapeDtypeStruct((width, hidden), bf16),
            jax.ShapeDtypeStruct((width, hidden), f32),
        ),
        in_specs=[
            pl.BlockSpec(memory_space=pltpu.SMEM),
            whole,
            whole,
            whole,
            piece,
            piece,
            piece,
            piece,
            column,
            pl.BlockSpec((block, width), lambda j: (j, 0)),
            column,
        ],
        out_specs=(column, column),
        scratch_shapes=[pltpu.VMEM((width, block), bf16), pltpu.VMEM((tokens, block), bf16)],
        cost_estimate=pl.CostEstimate(
            flops=6 * tokens * width * hidden,
            bytes_accessed=14 * width * hidden,
            transcendentals=tokens * hidden,
        ),
        name="grad_change",
    )(place, normed, turned, masked, *parts, tracker, w_out, grad_old)


def normed_of(hidden):
    widened = hidden.astype(f32)
    mean_square = jnp.mean(widened * widened, axis=-1, keepdims=True)
    return (widened * lax.rsqrt(mean_square + epsilon)).astype(bf16)


def shift(value, axis, step):
    count = lax.axis_size(axis)
    return lax.ppermute(value, axis, [(i, (i + step) % count) for i in range(count)])


def swap(value, bit):
    count = lax.axis_size("grp")
    return lax.ppermute(value, "grp", [(i, i ^ bit) for i in range(count)])


def stencil_taps(num_ref, den_ref):
    def wide(value):
        return jnp.full((8, 128), value, f32)

    weights = [
        wide(num_ref[t].astype(f32)) / wide(den_ref[t].astype(f32)) for t in range(ROUNDS)
    ]
    zero = wide(0.0)
    older = [wide(1.0)] + [zero] * ROUNDS
    current = older
    for t in range(ROUNDS):
        mean = []
        for d in range(ROUNDS + 1):
            left = current[d - 1] if d > 0 else current[1]
            right = current[d + 1] if d < ROUNDS else zero
            mean.append((left + current[d] + right) / 3.0)
        following = [weights[t] * m + (1.0 - weights[t]) * o for m, o in zip(mean, older)]
        older, current = current, following
    return current


def stencil_body(num_ref, den_ref, cells_ref, out_ref, wide_ref):
    workers, rows, _ = cells_ref.shape
    wide_ref[pl.ds(ROUNDS, workers)] = cells_ref[...].astype(f32)
    wide_ref[pl.ds(0, ROUNDS)] = cells_ref[pl.ds(workers - ROUNDS, ROUNDS)].astype(f32)
    wide_ref[pl.ds(ROUNDS + workers, ROUNDS)] = cells_ref[pl.ds(0, ROUNDS)].astype(f32)
    taps = [jnp.tile(t, (rows // 8, 1)) for t in stencil_taps(num_ref, den_ref)]

    def one(b, carry):
        total = taps[0] * wide_ref[b + ROUNDS]
        for d in range(1, ROUNDS + 1):
            total = total + taps[d] * (wide_ref[b + ROUNDS - d] + wide_ref[b + ROUNDS + d])
        out_ref[b] = total.astype(bf16)
        return carry

    lax.fori_loop(0, workers, one, 0, unroll=4)


def stencil(cells, cheb_num, cheb_den):
    workers, rows, lanes = cells.shape
    block = 24 if rows % 24 == 0 else rows
    spec = pl.BlockSpec((workers, block, lanes), lambda i: (0, i, 0))
    return pl.pallas_call(
        stencil_body,
        grid=(rows // block,),
        out_shape=jax.ShapeDtypeStruct(cells.shape, bf16),
        in_specs=[
            pl.BlockSpec(memory_space=pltpu.SMEM),
            pl.BlockSpec(memory_space=pltpu.SMEM),
            spec,
        ],
        out_specs=spec,
        scratch_shapes=[pltpu.VMEM((workers + 2 * ROUNDS, block, lanes), f32)],
        cost_estimate=pl.CostEstimate(
            flops=14 * cells.size, bytes_accessed=4 * cells.size, transcendentals=0
        ),
        name="stencil",
    )(cheb_num, cheb_den, cells)


def to_tiles(value, workers):
    rows, cols = value.shape
    tiles = value.reshape(rows // 8, 8, cols // 128, 128).transpose(0, 2, 1, 3)
    return tiles.reshape(workers, rows * cols // (128 * workers), 128)


def from_tiles(tiles, rows, cols):
    value = tiles.reshape(rows // 8, cols // 128, 8, 128).transpose(0, 2, 1, 3)
    return value.reshape(rows, cols)


def consensus_of(tracker, cheb_num, cheb_den):
    workers = lax.axis_size("blk")
    cells = to_tiles(tracker, workers)
    cells = lax.all_to_all(cells, "blk", 0, 0, tiled=True)
    cells = stencil(cells, cheb_num, cheb_den)
    cells = lax.all_to_all(cells, "blk", 0, 0, tiled=True)
    return from_tiles(cells, *tracker.shape)


def mixed_of(w_in):
    rows = w_in.shape[0]
    half, quarter = rows // 2, rows // 4
    member = lax.axis_index("grp")
    core, chip = member % 2, member // 2
    other = lax.dynamic_slice_in_dim(w_in, (1 - core) * half, half, 0)
    mine = lax.dynamic_slice_in_dim(w_in, core * half, half, 0)
    pair = mine.astype(f32) + swap(other, 1).astype(f32)
    other = lax.dynamic_slice_in_dim(pair, (1 - chip) * quarter, quarter, 0).astype(bf16)
    mine = lax.dynamic_slice_in_dim(pair, chip * quarter, quarter, 0)
    total = mine + swap(other, 2).astype(f32)
    sent = total.astype(bf16)
    below, above = shift(sent, "blk", 1), shift(sent, "blk", -1)
    mean = ((below.astype(f32) + total + above.astype(f32)) / 3.0 / 4.0).astype(bf16)
    far = swap(mean, 2)
    near = swap(mean, 1)
    last = swap(far, 1)
    place = jnp.stack(
        [
            core * 2 + chip,
            core * 2 + 1 - chip,
            (1 - core) * 2 + chip,
            (1 - core) * 2 + 1 - chip,
        ]
    ).astype(jnp.int32)
    return place, (mean, far, near, last)


def shards(hidden, cotangent, token_ids, w_in, w_out, tracker, grad_old, cheb_num, cheb_den):
    consensus = consensus_of(tracker[0, 0], cheb_num, cheb_den)
    place, parts = mixed_of(w_in[0, 0])
    normed = normed_of(hidden)
    masked = jnp.where((token_ids != 0)[:, None], cotangent, jnp.zeros_like(cotangent))
    normed, turned, masked = lax.optimization_barrier((normed, normed.T, masked))
    new_params, change = grad_change(
        place, normed, turned, masked, parts, tracker[0, 0], w_out, grad_old[0, 0]
    )
    new_tracker = (consensus.astype(f32) + change).astype(bf16)
    return (new_params[None, None], new_tracker[None, None])


def solution(mesh):
    placed = (
        P(("blk", "grp"), None),
        P(("blk", "grp"), None),
        P(("blk", "grp")),
        P("blk", "grp", None, None),
        P(),
        P("blk", "grp", None, None),
        P("blk", "grp", None, None),
        P(),
        P(),
    )
    return jax.shard_map(
        shards,
        mesh=mesh,
        in_specs=placed,
        out_specs=(P("blk", "grp", None, None), P("blk", "grp", None, None)),
        check_vma=False,
    )
```

```python
import math

import jax
import jax.numpy as jnp
from jax import lax
from jax.experimental import pallas as pl
from jax.experimental.pallas import tpu as pltpu
from jax.sharding import PartitionSpec as P


ROUNDS = 4
SPAN = 16
LAG = 450

epsilon = 1e-06
step_size = 0.25
tanh_scale = math.sqrt(2.0 / math.pi)

f32 = jnp.float32
bf16 = jnp.bfloat16


def slope_of(scaled, back_flow, inv_root):
    lead, bend = tanh_scale * inv_root, tanh_scale * 0.044715 * inv_root**3
    square = scaled * scaled
    half = 0.5 * jnp.tanh(scaled * (lead + bend * square)) + 0.5
    inner = scaled * (2.0 * lead + 6.0 * bend * square)
    return back_flow * (half + half * (1.0 - half) * inner)


def grad_body(
    member_ref,
    normed_ref,
    turned_ref,
    masked_ref,
    first_ref,
    second_ref,
    third_ref,
    fourth_ref,
    tracker_ref,
    w_out_ref,
    old_ref,
    params_ref,
    out_ref,
    mixed_ref,
    slope_ref,
):
    tokens, width = normed_ref.shape
    inv_root = width ** (-0.5)
    quarter = width // 4
    core, chip = member_ref[0] & 1, member_ref[0] >> 1
    places = (
        core * 2 + chip,
        core * 2 + 1 - chip,
        (1 - core) * 2 + chip,
        (1 - core) * 2 + 1 - chip,
    )
    for place, part_ref in zip(places, (first_ref, second_ref, third_ref, fourth_ref)):
        at = pl.multiple_of(place * quarter, quarter)
        mixed_ref[pl.ds(at, quarter)] = part_ref[...]
    params_ref[...] = (
        mixed_ref[...].astype(f32) - step_size * tracker_ref[...].astype(f32)
    ).astype(bf16)
    step = 256
    held = None
    for at in range(0, tokens + step, step):
        ready = held
        if at < tokens:
            rows = pl.ds(at, step)
            scaled = jnp.dot(normed_ref[rows], params_ref[...], preferred_element_type=f32)
            back_flow = lax.dot_general(
                masked_ref[rows],
                w_out_ref[...],
                (((1,), (1,)), ((), ())),
                preferred_element_type=f32,
            )
            held = (rows, scaled, back_flow)
        if ready is not None:
            rows, scaled, back_flow = ready
            slope_ref[rows] = slope_of(scaled, back_flow, inv_root).astype(bf16)
    grad = jnp.dot(turned_ref[...], slope_ref[...], preferred_element_type=f32)
    out_ref[...] = grad * inv_root - old_ref[...].astype(f32)


def grad_change(member, normed, turned, masked, parts, tracker, w_out, grad_old):
    tokens, width = normed.shape
    hidden = tracker.shape[1]
    block = 256
    whole = pl.BlockSpec(memory_space=pltpu.VMEM)
    column = pl.BlockSpec((width, block), lambda j: (0, j))
    piece = pl.BlockSpec((width // 4, block), lambda j: (0, j))
    return pl.pallas_call(
        grad_body,
        grid=(hidden // block,),
        out_shape=(
            jax.ShapeDtypeStruct((width, hidden), bf16),
            jax.ShapeDtypeStruct((width, hidden), f32),
        ),
        in_specs=[
            pl.BlockSpec(memory_space=pltpu.SMEM),
            whole,
            whole,
            whole,
            piece,
            piece,
            piece,
            piece,
            column,
            pl.BlockSpec((block, width), lambda j: (j, 0)),
            column,
        ],
        out_specs=(column, column),
        scratch_shapes=[pltpu.VMEM((width, block), bf16), pltpu.VMEM((tokens, block), bf16)],
        cost_estimate=pl.CostEstimate(
            flops=6 * tokens * width * hidden,
            bytes_accessed=14 * width * hidden,
            transcendentals=tokens * hidden,
        ),
        name="grad_change",
    )(member, normed, turned, masked, *parts, tracker, w_out, grad_old)


def normed_of(hidden):
    widened = hidden.astype(f32)
    mean_square = jnp.mean(widened * widened, axis=-1, keepdims=True)
    return (widened * lax.rsqrt(mean_square + epsilon)).astype(bf16)


def shift(value, axis, step):
    count = lax.axis_size(axis)
    return lax.ppermute(value, axis, [(i, (i + step) % count) for i in range(count)])


def swap(value, bit):
    count = lax.axis_size("grp")
    return lax.ppermute(value, "grp", [(i, i ^ bit) for i in range(count)])


def taps_body(lag_ref, num_ref, den_ref, taps_ref):
    def wide(value):
        return jnp.full((8, 128), value, f32)

    zero = wide(0.0)

    def once(_, carry):
        older = [wide(1.0)] + [zero] * ROUNDS
        current = older
        for t in range(ROUNDS):
            weight = wide(num_ref[t].astype(f32)) / wide(den_ref[t].astype(f32))
            mean = []
            for d in range(ROUNDS + 1):
                left = current[d - 1] if d > 0 else current[1]
                right = current[d + 1] if d < ROUNDS else zero
                mean.append((left + current[d] + right) / 3.0)
            following = [weight * m + (1.0 - weight) * o for m, o in zip(mean, older)]
            older, current = current, following
        for d in range(ROUNDS + 1):
            taps_ref[d] = current[d]
        return carry

    lax.fori_loop(0, 1 + lag_ref[0], once, 0)


def stencil_taps(lag, cheb_num, cheb_den):
    scalars = pl.BlockSpec(memory_space=pltpu.SMEM)
    return pl.pallas_call(
        taps_body,
        out_shape=jax.ShapeDtypeStruct((ROUNDS + 1, 8, 128), f32),
        in_specs=[scalars, scalars, scalars],
        out_specs=pl.BlockSpec(memory_space=pltpu.VMEM),
        name="stencil_taps",
    )(lag, cheb_num, cheb_den)


def stencil_body(taps_ref, below_ref, cells_ref, above_ref, out_ref, wide_ref):
    workers, rows, lanes = cells_ref.shape
    wide_ref[pl.ds(0, ROUNDS)] = below_ref[...].astype(f32)
    wide_ref[pl.ds(ROUNDS, workers)] = cells_ref[...].astype(f32)
    wide_ref[pl.ds(ROUNDS + workers, ROUNDS)] = above_ref[...].astype(f32)
    taps = [taps_ref[d] for d in range(ROUNDS + 1)]

    def one(b, carry):
        for row in range(0, rows, 8):
            for lane in range(0, lanes, 128):
                at = (pl.ds(row, 8), pl.ds(lane, 128))
                total = taps[0] * wide_ref[b + ROUNDS, *at]
                for d in range(1, ROUNDS + 1):
                    pair = wide_ref[b + ROUNDS - d, *at] + wide_ref[b + ROUNDS + d, *at]
                    total = total + taps[d] * pair
                out_ref[b, *at] = total.astype(bf16)
        return carry

    lax.fori_loop(0, workers, one, 0)


def stencil(taps, below, cells, above):
    workers, rows, lanes = cells.shape
    block = 1536
    spec = pl.BlockSpec((workers, rows, block), lambda i: (0, 0, i))
    side = pl.BlockSpec((ROUNDS, rows, block), lambda i: (0, 0, i))
    return pl.pallas_call(
        stencil_body,
        grid=(lanes // block,),
        out_shape=jax.ShapeDtypeStruct(cells.shape, bf16),
        in_specs=[pl.BlockSpec(memory_space=pltpu.VMEM), side, spec, side],
        out_specs=spec,
        scratch_shapes=[pltpu.VMEM((workers + 2 * ROUNDS, rows, block), f32)],
        cost_estimate=pl.CostEstimate(
            flops=14 * cells.size, bytes_accessed=4 * cells.size, transcendentals=0
        ),
        name="stencil",
    )(taps, below, cells, above)


def traded(cells):
    count = lax.axis_size("blk")
    groups = [list(range(at, at + SPAN)) for at in range(0, count, SPAN)]
    return lax.all_to_all(cells, "blk", 0, 0, tiled=True, axis_index_groups=groups)


def consensus_of(tracker, taps):
    rows, cols = tracker.shape
    cells = tracker.reshape(SPAN, rows // SPAN, cols)
    cells = traded(cells)
    below = shift(cells[SPAN - ROUNDS :], "blk", SPAN)
    above = shift(cells[:ROUNDS], "blk", -SPAN)
    cells = stencil(taps, below, cells, above)
    cells = traded(cells)
    return cells.reshape(rows, cols)


def mixed_of(w_in):
    rows = w_in.shape[0]
    half, quarter = rows // 2, rows // 4
    member = lax.axis_index("grp")
    core, chip = member % 2, member // 2
    other = lax.dynamic_slice_in_dim(w_in, (1 - core) * half, half, 0)
    mine = lax.dynamic_slice_in_dim(w_in, core * half, half, 0)
    pair = mine.astype(f32) + swap(other, 1).astype(f32)
    other = lax.dynamic_slice_in_dim(pair, (1 - chip) * quarter, quarter, 0).astype(bf16)
    mine = lax.dynamic_slice_in_dim(pair, chip * quarter, quarter, 0)
    total = mine + swap(other, 2).astype(f32)
    sent = total.astype(bf16)
    below, above = shift(sent, "blk", 1), shift(sent, "blk", -1)
    mean = ((below.astype(f32) + total + above.astype(f32)) / 3.0 / 4.0).astype(bf16)
    far = swap(mean, 2)
    near = swap(mean, 1)
    last = swap(far, 1)
    return member.astype(jnp.int32).reshape(1), (mean, far, near, last)


def shards(hidden, cotangent, token_ids, w_in, w_out, tracker, grad_old, cheb_num, cheb_den):
    lag = (lax.axis_index("grp") % 2 * LAG).astype(jnp.int32).reshape(1)
    taps = stencil_taps(lag, cheb_num, cheb_den)
    consensus = consensus_of(tracker[0, 0], taps)
    member, parts = mixed_of(w_in[0, 0])
    normed = normed_of(hidden)
    masked = jnp.where((token_ids != 0)[:, None], cotangent, jnp.zeros_like(cotangent))
    normed, turned, masked = lax.optimization_barrier((normed, normed.T, masked))
    new_params, change = grad_change(
        member, normed, turned, masked, parts, tracker[0, 0], w_out, grad_old[0, 0]
    )
    new_tracker = (consensus.astype(f32) + change).astype(bf16)
    return (new_params[None, None], new_tracker[None, None])


def solution(mesh):
    placed = (
        P(("blk", "grp"), None),
        P(("blk", "grp"), None),
        P(("blk", "grp")),
        P("blk", "grp", None, None),
        P(),
        P("blk", "grp", None, None),
        P("blk", "grp", None, None),
        P(),
        P(),
    )
    return jax.shard_map(
        shards,
        mesh=mesh,
        in_specs=placed,
        out_specs=(P("blk", "grp", None, None), P("blk", "grp", None, None)),
        check_vma=False,
    )
```

```python
import math

import jax
import jax.numpy as jnp
from jax import lax
from jax.experimental import pallas as pl
from jax.experimental.pallas import tpu as pltpu
from jax.sharding import PartitionSpec as P


ROUNDS = 4
SPAN = 16
LAG = 450

epsilon = 1e-06
step_size = 0.25
tanh_scale = math.sqrt(2.0 / math.pi)

f32 = jnp.float32
bf16 = jnp.bfloat16


def slope_of(scaled, back_flow, inv_root):
    lead, bend = tanh_scale * inv_root, tanh_scale * 0.044715 * inv_root**3
    square = scaled * scaled
    half = 0.5 * jnp.tanh(scaled * (lead + bend * square)) + 0.5
    inner = scaled * (2.0 * lead + 6.0 * bend * square)
    return back_flow * (half + half * (1.0 - half) * inner)


def grad_body(
    member_ref,
    normed_ref,
    turned_ref,
    masked_ref,
    first_ref,
    second_ref,
    third_ref,
    fourth_ref,
    tracker_ref,
    w_out_ref,
    old_ref,
    params_ref,
    out_ref,
    mixed_ref,
    slope_ref,
):
    tokens, width = normed_ref.shape
    inv_root = width ** (-0.5)
    quarter = width // 4
    core, chip = member_ref[0] & 1, member_ref[0] >> 1
    places = (
        core * 2 + chip,
        core * 2 + 1 - chip,
        (1 - core) * 2 + chip,
        (1 - core) * 2 + 1 - chip,
    )
    for place, part_ref in zip(places, (first_ref, second_ref, third_ref, fourth_ref)):
        at = pl.multiple_of(place * quarter, quarter)
        mixed_ref[pl.ds(at, quarter)] = part_ref[...]
    params_ref[...] = (
        mixed_ref[...].astype(f32) - step_size * tracker_ref[...].astype(f32)
    ).astype(bf16)
    step = 256
    held = None
    for at in range(0, tokens + step, step):
        ready = held
        if at < tokens:
            rows = pl.ds(at, step)
            scaled = jnp.dot(normed_ref[rows], params_ref[...], preferred_element_type=f32)
            back_flow = lax.dot_general(
                masked_ref[rows],
                w_out_ref[...],
                (((1,), (1,)), ((), ())),
                preferred_element_type=f32,
            )
            held = (rows, scaled, back_flow)
        if ready is not None:
            rows, scaled, back_flow = ready
            slope_ref[rows] = slope_of(scaled, back_flow, inv_root).astype(bf16)
    grad = jnp.dot(turned_ref[...], slope_ref[...], preferred_element_type=f32)
    out_ref[...] = (grad * inv_root - old_ref[...].astype(f32)).astype(bf16)


def grad_change(member, normed, turned, masked, parts, tracker, w_out, grad_old):
    tokens, width = normed.shape
    hidden = tracker.shape[1]
    block = 512
    whole = pl.BlockSpec(memory_space=pltpu.VMEM)
    column = pl.BlockSpec((width, block), lambda j: (0, j))
    piece = pl.BlockSpec((width // 4, block), lambda j: (0, j))
    return pl.pallas_call(
        grad_body,
        grid=(hidden // block,),
        out_shape=(
            jax.ShapeDtypeStruct((width, hidden), bf16),
            jax.ShapeDtypeStruct((width, hidden), bf16),
        ),
        in_specs=[
            pl.BlockSpec(memory_space=pltpu.SMEM),
            whole,
            whole,
            whole,
            piece,
            piece,
            piece,
            piece,
            column,
            pl.BlockSpec((block, width), lambda j: (j, 0)),
            column,
        ],
        out_specs=(column, column),
        scratch_shapes=[pltpu.VMEM((width, block), bf16), pltpu.VMEM((tokens, block), bf16)],
        cost_estimate=pl.CostEstimate(
            flops=6 * tokens * width * hidden,
            bytes_accessed=14 * width * hidden,
            transcendentals=tokens * hidden,
        ),
        name="grad_change",
    )(member, normed, turned, masked, *parts, tracker, w_out, grad_old)


def normed_of(hidden):
    widened = hidden.astype(f32)
    mean_square = jnp.mean(widened * widened, axis=-1, keepdims=True)
    return (widened * lax.rsqrt(mean_square + epsilon)).astype(bf16)


def shift(value, axis, step):
    count = lax.axis_size(axis)
    return lax.ppermute(value, axis, [(i, (i + step) % count) for i in range(count)])


def swap(value, bit):
    count = lax.axis_size("grp")
    return lax.ppermute(value, "grp", [(i, i ^ bit) for i in range(count)])


def taps_body(lag_ref, num_ref, den_ref, taps_ref):
    def wide(value):
        return jnp.full((8, 128), value, f32)

    zero = wide(0.0)

    def once(_, carry):
        older = [wide(1.0)] + [zero] * ROUNDS
        current = older
        for t in range(ROUNDS):
            weight = wide(num_ref[t].astype(f32)) / wide(den_ref[t].astype(f32))
            mean = []
            for d in range(ROUNDS + 1):
                left = current[d - 1] if d > 0 else current[1]
                right = current[d + 1] if d < ROUNDS else zero
                mean.append((left + current[d] + right) / 3.0)
            following = [weight * m + (1.0 - weight) * o for m, o in zip(mean, older)]
            older, current = current, following
        for d in range(ROUNDS + 1):
            taps_ref[d] = current[d]
        return carry

    lax.fori_loop(0, 1 + lag_ref[0], once, 0)


def stencil_taps(lag, cheb_num, cheb_den):
    scalars = pl.BlockSpec(memory_space=pltpu.SMEM)
    return pl.pallas_call(
        taps_body,
        out_shape=jax.ShapeDtypeStruct((ROUNDS + 1, 8, 128), f32),
        in_specs=[scalars, scalars, scalars],
        out_specs=pl.BlockSpec(memory_space=pltpu.VMEM),
        name="stencil_taps",
    )(lag, cheb_num, cheb_den)


def stencil_body(taps_ref, below_ref, cells_ref, above_ref, out_ref, wide_ref):
    workers, rows, lanes = cells_ref.shape
    wide_ref[pl.ds(0, ROUNDS)] = below_ref[...].astype(f32)
    wide_ref[pl.ds(ROUNDS, workers)] = cells_ref[...].astype(f32)
    wide_ref[pl.ds(ROUNDS + workers, ROUNDS)] = above_ref[...].astype(f32)
    taps = [taps_ref[d] for d in range(ROUNDS + 1)]

    def one(b, carry):
        for row in range(0, rows, 8):
            for lane in range(0, lanes, 128):
                at = (pl.ds(row, 8), pl.ds(lane, 128))
                total = taps[0] * wide_ref[b + ROUNDS, *at]
                for d in range(1, ROUNDS + 1):
                    pair = wide_ref[b + ROUNDS - d, *at] + wide_ref[b + ROUNDS + d, *at]
                    total = total + taps[d] * pair
                out_ref[b, *at] = total.astype(bf16)
        return carry

    lax.fori_loop(0, workers, one, 0)


def stencil(taps, below, cells, above):
    workers, rows, lanes = cells.shape
    block = 1536
    spec = pl.BlockSpec((workers, rows, block), lambda i: (0, 0, i))
    side = pl.BlockSpec((ROUNDS, rows, block), lambda i: (0, 0, i))
    return pl.pallas_call(
        stencil_body,
        grid=(lanes // block,),
        out_shape=jax.ShapeDtypeStruct(cells.shape, bf16),
        in_specs=[pl.BlockSpec(memory_space=pltpu.VMEM), side, spec, side],
        out_specs=spec,
        scratch_shapes=[pltpu.VMEM((workers + 2 * ROUNDS, rows, block), f32)],
        cost_estimate=pl.CostEstimate(
            flops=14 * cells.size, bytes_accessed=4 * cells.size, transcendentals=0
        ),
        name="stencil",
    )(taps, below, cells, above)


def traded(cells):
    count = lax.axis_size("blk")
    groups = [list(range(at, at + SPAN)) for at in range(0, count, SPAN)]
    return lax.all_to_all(cells, "blk", 0, 0, tiled=True, axis_index_groups=groups)


def consensus_of(tracker, taps):
    rows, cols = tracker.shape
    cells = tracker.reshape(SPAN, rows // SPAN, cols)
    cells = traded(cells)
    below = shift(cells[SPAN - ROUNDS :], "blk", SPAN)
    above = shift(cells[:ROUNDS], "blk", -SPAN)
    cells = stencil(taps, below, cells, above)
    cells = traded(cells)
    return cells.reshape(rows, cols)


def mixed_of(w_in):
    rows = w_in.shape[0]
    half, quarter = rows // 2, rows // 4
    member = lax.axis_index("grp")
    core, chip = member % 2, member // 2
    other = lax.dynamic_slice_in_dim(w_in, (1 - core) * half, half, 0)
    mine = lax.dynamic_slice_in_dim(w_in, core * half, half, 0)
    pair = mine.astype(f32) + swap(other, 1).astype(f32)
    other = lax.dynamic_slice_in_dim(pair, (1 - chip) * quarter, quarter, 0).astype(bf16)
    mine = lax.dynamic_slice_in_dim(pair, chip * quarter, quarter, 0)
    total = mine + swap(other, 2).astype(f32)
    sent = total.astype(bf16)
    below, above = shift(sent, "blk", 1), shift(sent, "blk", -1)
    mean = ((below.astype(f32) + total + above.astype(f32)) / 3.0 / 4.0).astype(bf16)
    far = swap(mean, 2)
    near = swap(mean, 1)
    last = swap(far, 1)
    return member.astype(jnp.int32).reshape(1), (mean, far, near, last)


def shards(hidden, cotangent, token_ids, w_in, w_out, tracker, grad_old, cheb_num, cheb_den):
    lag = (lax.axis_index("grp") % 2 * LAG).astype(jnp.int32).reshape(1)
    taps = stencil_taps(lag, cheb_num, cheb_den)
    consensus = consensus_of(tracker[0, 0], taps)
    member, parts = mixed_of(w_in[0, 0])
    normed = normed_of(hidden)
    masked = jnp.where((token_ids != 0)[:, None], cotangent, jnp.zeros_like(cotangent))
    normed, turned, masked = lax.optimization_barrier((normed, normed.T, masked))
    new_params, change = grad_change(
        member, normed, turned, masked, parts, tracker[0, 0], w_out, grad_old[0, 0]
    )
    new_tracker = (consensus.astype(f32) + change.astype(f32)).astype(bf16)
    return (new_params[None, None], new_tracker[None, None])


def solution(mesh):
    placed = (
        P(("blk", "grp"), None),
        P(("blk", "grp"), None),
        P(("blk", "grp")),
        P("blk", "grp", None, None),
        P(),
        P("blk", "grp", None, None),
        P("blk", "grp", None, None),
        P(),
        P(),
    )
    return jax.shard_map(
        shards,
        mesh=mesh,
        in_specs=placed,
        out_specs=(P("blk", "grp", None, None), P("blk", "grp", None, None)),
        check_vma=False,
    )
```
